32 devices in a mesh: doc: 4 (over z), term: 8 (over y, x, core).
Axes of the slice: x: 2, y: 2, z: 4, core: 2. Of those that a mesh axis runs over, the one named last changes fastest.
Arguments:
- tiles: bfloat16 [4, 8, 8, 512, 512], P('doc', 'term'), may hold values from 0.0009994507 to 1
- tile_rows: int32 [4, 8, 8], P('doc', 'term'), may hold values from 0 to 31, as said below
- tile_cols: int32 [4, 8, 8], P('doc', 'term'), may hold values from 0 to 63
- counts: int32 [4, 8], P('doc', 'term'), may hold values from 2 to 8, as said below
- start_block: float32 [16, 262144], P(None, 'term'), may hold values from -6 to 6
Outputs:
- left_block: float32 [16, 65536], P(None, ('doc', 'term'))
- right_block: float32 [16, 262144], P(None, ('term', 'doc'))
- coefficients: float32 [5, 16, 16], replicated
The draws below stay inside these ranges and needn't reach their ends.
Inputs may be any that keep to these rules, and one draw needn't show every extreme that they name: On each device the pairs (tile_rows, tile_cols) of its 8 slots are distinct. `counts`: some device uses all 8 slots.
All inputs are finite; a program needn't handle non-finite values.
Results may differ from the reference program's by a relative error of at most 0.0031.
Values sent between devices are 32-bit elements; how exact they have to be, the bound alone decides.
No kernel may reach another device: no remote copies, remote signals or barrier semaphores. Data moves between devices by JAX's collectives and lax.ppermute only.
A program may use at most 64 MiB of HBM per device.

```python
import math
import jax
import jax.numpy as jnp
from jax import lax

TILE = 512
BLOCK = 16
TERM_TILES = 64
DOC_TILES = 32
SLOTS = 8
NTERM = 262144
N_DOC = 4
N_TERM = 8


def pick_slots(subkey):
    return jax.random.permutation(subkey, DOC_TILES * TERM_TILES)[:SLOTS]


def tile_positions(key):
    subkeys = jax.random.split(jax.random.fold_in(key, 11), N_DOC * N_TERM)
    picked = jax.vmap(pick_slots)(subkeys)
    return picked.reshape(N_DOC, N_TERM, SLOTS).astype(jnp.int32)


def draw_tile_rows(key, part):
    return (tile_positions(key) // TERM_TILES).astype(jnp.int32)


def draw_tile_cols(key, part):
    return (tile_positions(key) % TERM_TILES).astype(jnp.int32)


def draw_counts(key, part):
    devices = N_DOC * N_TERM
    base = jax.random.randint(jax.random.fold_in(key, 5), (devices,), SLOTS // 4, SLOTS + 1)
    chosen = jax.random.randint(jax.random.fold_in(key, 6), (), 0, devices)
    filled = jnp.where(jnp.arange(devices) == chosen, SLOTS, base)
    return filled.reshape(N_DOC, N_TERM).astype(jnp.int32)


def shard_levels(key, shape, shards, least, top_value):
    def one(dim, shards_of):
        draws = jax.random.uniform(jax.random.fold_in(jax.random.fold_in(key, 6), dim), (shards_of,), jnp.float32, least / len(shards), top_value / len(shards))
        return jnp.repeat(jnp.exp(draws), shape[dim] // shards_of).reshape((-1,) + (1,) * (len(shape) - dim - 1))

    loudness = one(*shards[0])
    for cut in shards[1:]:
        loudness = loudness * one(*cut)
    return loudness


def bell_draw(rng, shape, deviation, most, shards=(), held_as=jnp.bfloat16):
    array = deviation * jax.random.normal(rng, shape, jnp.float32)
    if shards:
        array = array * shard_levels(rng, shape, shards, -0.22, 0.18)
    return jnp.clip(array, -most, most).astype(held_as)


def setup_inputs(seed: int = 0) -> dict:
    splits = jax.random.split(jax.random.key(seed), 6)
    return {
        "tiles": jnp.clip(jnp.exp(math.log(1.0) - 6.9083047 * jax.random.uniform(splits[0], (N_DOC, N_TERM, SLOTS, TILE, TILE), jnp.float32) ** shard_levels(splits[0], (N_DOC, N_TERM, SLOTS, TILE, TILE), ((0, 4), (1, 8)), -0.2, 0.2)), 0.0009994507, 1.0).astype(jnp.bfloat16),
        "tile_rows": draw_tile_rows(jax.random.fold_in(splits[5], 71), 0),
        "tile_cols": draw_tile_cols(jax.random.fold_in(splits[5], 71), 0),
        "counts": draw_counts(jax.random.fold_in(splits[5], 71), 0),
        "start_block": bell_draw(splits[4], (BLOCK, NTERM), 1.0, 6.0, ((1, 8),), jnp.float32),
    }


def orthonormal(vectors, total_rows):
    highest = lax.Precision.HIGHEST
    gram_matrix = jnp.dot(vectors, vectors.T, precision=highest) / total_rows
    factor = jnp.linalg.cholesky(gram_matrix)
    return (jax.scipy.linalg.solve_triangular(factor, vectors, lower=True), factor)

def projected(vectors, earlier, total_rows):
    highest = lax.Precision.HIGHEST
    projection = jnp.dot(vectors, earlier.T, precision=highest) / total_rows
    return (vectors - jnp.dot(projection, earlier, precision=highest), projection)

def reference(tiles, tile_rows, tile_cols, counts, start_block):
    highest = lax.Precision.HIGHEST
    n_docs = N_DOC * DOC_TILES * TILE
    n_terms = N_TERM * TERM_TILES * TILE
    devices = N_DOC * N_TERM
    active = (jnp.arange(SLOTS)[None, None, :] < counts[:, :, None]).astype(jnp.float32)
    row_onehot = (tile_rows[..., None] == jnp.arange(DOC_TILES)[None, None, None, :]).astype(jnp.float32)
    col_onehot = (tile_cols[..., None] == jnp.arange(TERM_TILES)[None, None, None, :]).astype(jnp.float32)
    row_live = row_onehot * active[..., None]
    col_live = col_onehot * active[..., None]

    def device_degrees(index):
        doc_index = index // N_TERM
        term_index = index % N_TERM
        values = tiles[doc_index, term_index].astype(jnp.float32)
        row_sums = lax.optimization_barrier(jnp.sum(values, axis=2))
        col_sums = lax.optimization_barrier(jnp.sum(values, axis=1))
        row_part = jnp.einsum('kr,ka->ra', row_live[doc_index, term_index], row_sums, precision=highest)
        col_part = jnp.einsum('kc,kb->cb', col_live[doc_index, term_index], col_sums, precision=highest)
        return (row_part.reshape(-1), col_part.reshape(-1))
    row_parts, col_parts = lax.map(device_degrees, jnp.arange(devices))
    row_degree = 1.0 + lax.optimization_barrier(jnp.sum(row_parts.reshape(N_DOC, N_TERM, -1), axis=1)).reshape(-1)
    col_degree = 1.0 + lax.optimization_barrier(jnp.sum(col_parts.reshape(N_DOC, N_TERM, -1), axis=0)).reshape(-1)
    row_scale = lax.rsqrt(row_degree)
    col_scale = lax.rsqrt(col_degree)

    def forward(right_block):
        scaled = (right_block * col_scale[None, :]).astype(jnp.bfloat16).astype(jnp.float32)
        scaled = scaled.reshape(BLOCK, N_TERM, TERM_TILES, TILE)

        def device_forward(index):
            doc_index = index // N_TERM
            term_index = index % N_TERM
            local_right = scaled[:, term_index]
            pieces = jnp.einsum('kc,bcx->kbx', col_onehot[doc_index, term_index], local_right, precision=highest)
            values = tiles[doc_index, term_index].astype(jnp.float32)
            product = jnp.einsum('kab,kcb->kca', values, pieces, precision=highest)
            return jnp.einsum('kr,kca->cra', row_live[doc_index, term_index], product, precision=highest).reshape(BLOCK, -1)
        parts = lax.map(device_forward, jnp.arange(devices))
        summed = lax.optimization_barrier(jnp.sum(parts.reshape(N_DOC, N_TERM, BLOCK, -1), axis=1))
        return summed.transpose(1, 0, 2).reshape(BLOCK, -1) * row_scale[None, :]

    def backward(left_block):
        scaled = (left_block * row_scale[None, :]).astype(jnp.bfloat16).astype(jnp.float32)
        scaled = scaled.reshape(BLOCK, N_DOC, DOC_TILES, TILE)

        def device_backward(index):
            doc_index = index // N_TERM
            term_index = index % N_TERM
            local_left = scaled[:, doc_index]
            pieces = jnp.einsum('kr,brx->kbx', row_onehot[doc_index, term_index], local_left, precision=highest)
            values = tiles[doc_index, term_index].astype(jnp.float32)
            product = jnp.einsum('kab,kca->kcb', values, pieces, precision=highest)
            return jnp.einsum('kc,kxb->xcb', col_live[doc_index, term_index], product, precision=highest).reshape(BLOCK, -1)
        parts = lax.map(device_backward, jnp.arange(devices))
        summed = lax.optimization_barrier(jnp.sum(parts.reshape(N_DOC, N_TERM, BLOCK, -1), axis=0))
        return summed.transpose(1, 0, 2).reshape(BLOCK, -1) * col_scale[None, :]
    first_right, factor_zero = orthonormal(start_block, n_terms)
    left_one, factor_one = orthonormal(forward(first_right), n_docs)
    right_raw, projection_one = projected(backward(left_one), first_right, n_terms)
    right_two, factor_two = orthonormal(right_raw, n_terms)
    left_raw, projection_two = projected(forward(right_two), left_one, n_docs)
    left_two, factor_three = orthonormal(left_raw, n_docs)
    coefficients = jnp.stack([factor_one, projection_one, factor_two, projection_two, factor_three])
    return (left_two, right_two, coefficients)
```

```python
import functools

import jax
import jax.numpy as jnp
from jax import lax
from jax.experimental import pallas as pl
from jax.experimental.pallas import tpu as pltpu
from jax.sharding import PartitionSpec as P

TERM_TILES = 64
DOC_TILES = 32
LANES = 128
F32 = jnp.float32
BF16 = jnp.bfloat16
HIGHEST = lax.Precision.HIGHEST
VMEM = pltpu.MemorySpace.VMEM
SMEM = pltpu.MemorySpace.SMEM


def nn(a, b, precision=None):
    return lax.dot_general(
        a, b, (((1,), (0,)), ((), ())), precision=precision, preferred_element_type=F32
    )


def nt(a, b, precision=None):
    return lax.dot_general(
        a, b, (((1,), (1,)), ((), ())), precision=precision, preferred_element_type=F32
    )


def split2(x):
    high = x.astype(BF16)
    return jnp.concatenate([high, (x - high.astype(F32)).astype(BF16)], axis=0)


def split3(x):
    high = x.astype(BF16)
    rest = x - high.astype(F32)
    middle = rest.astype(BF16)
    low = (rest - middle.astype(F32)).astype(BF16)
    return jnp.concatenate([high, middle, low], axis=0)


def fold3(gram, edge):
    rows = gram[:edge] + gram[edge : 2 * edge] + gram[2 * edge :]
    return rows[:, :edge] + rows[:, edge : 2 * edge] + rows[:, 2 * edge :]


def pad_lanes(x):
    return jnp.concatenate([x, jnp.zeros((x.shape[0], LANES - x.shape[1]), F32)], axis=1)


def column_sums_body(cols, in_use, tile, start, sums, picked):
    slot = pl.program_id(0)
    edge = tile.shape[1]
    total = nn(jnp.ones((16, edge), BF16), tile[0])[0:1]
    live = slot < in_use[0]
    mark = jnp.where(live, cols[slot], -1).astype(F32)
    total = jnp.concatenate([jnp.where(live, total, 0.0), jnp.full((1, LANES), mark, F32)], axis=1)
    index = lax.broadcasted_iota(jnp.int32, sums.shape, 0)
    sums[...] = jnp.where(index == slot, total, sums[...])
    picked[0] = start[...]


def column_sums(tiles, start, cols, in_use):
    slots, edge, _ = tiles.shape
    vectors = start.shape[0]
    return pl.pallas_call(
        column_sums_body,
        grid_spec=pltpu.PrefetchScalarGridSpec(
            num_scalar_prefetch=2,
            grid=(slots,),
            in_specs=[
                pl.BlockSpec((1, edge, edge), lambda s, c, u: (s, 0, 0)),
                pl.BlockSpec((vectors, edge), lambda s, c, u: (0, c[s])),
            ],
            out_specs=[
                pl.BlockSpec((slots, edge + LANES), lambda s, c, u: (0, 0)),
                pl.BlockSpec((1, vectors, edge), lambda s, c, u: (s, 0, 0)),
            ],
        ),
        out_shape=[
            jax.ShapeDtypeStruct((slots, edge + LANES), F32),
            jax.ShapeDtypeStruct((slots, vectors, edge), F32),
        ],
        name="column_sums",
    )(cols, in_use, tiles, start)


def start_gram_body(start, gram, total):
    step = pl.program_id(0)
    vectors = start.shape[0]
    pieces = split3(start[...])
    part = nt(pieces, pieces)

    @pl.when(step == 0)
    def _():
        total[...] = part

    @pl.when(step > 0)
    def _():
        total[...] += part

    @pl.when(step == pl.num_programs(0) - 1)
    def _():
        gram[...] = pad_lanes(fold3(total[...], vectors))


def start_gram(start):
    vectors, count = start.shape
    chunk = count // 8
    return pl.pallas_call(
        start_gram_body,
        grid=(8,),
        in_specs=[pl.BlockSpec((vectors, chunk), lambda s: (0, s))],
        out_specs=pl.BlockSpec((vectors, LANES), lambda s: (0, 0)),
        out_shape=jax.ShapeDtypeStruct((vectors, LANES), F32),
        scratch_shapes=[pltpu.VMEM((3 * vectors, 3 * vectors), F32)],
        name="start_gram",
    )(start)


def first_forward_body(groups, *refs):
    rows, cols, in_use = refs[:3]
    tiles, picked, gram = refs[3:6]
    sums = refs[6 : 6 + groups]
    payload, col_scale = refs[6 + groups :]
    copies = payload.shape[0]
    slots, vectors, edge = picked.shape
    base = slots * vectors
    half = gram.shape[0] // 2
    values = [r[:, 0:edge] for r in sums]
    marks = [r[:, edge : edge + LANES] for r in sums]
    for s in range(slots):
        column = cols[s].astype(F32)
        degree = jnp.ones((1, edge), F32)
        for value, mark in zip(values, marks):
            same = jnp.where(mark == column, 1.0, 0.0)
            same = jnp.concatenate([same] * (edge // LANES), axis=1)
            degree = degree + jnp.sum(same * value, axis=0, keepdims=True)
        scale = lax.rsqrt(degree)
        col_scale[s : s + 1, :] = scale
        left = jnp.concatenate(
            [split2(picked[s] * scale), jnp.ones((vectors, edge), BF16)], axis=0
        )
        out = nt(left, tiles[s])
        product = out[:vectors] + out[vectors : 2 * vectors]
        for q in range(copies):
            payload[q, s * vectors : (s + 1) * vectors, :] = product
            payload[q, base + s : base + s + 1, :] = out[2 * vectors : 2 * vectors + 1]
        mark = jnp.where(s < in_use[0], rows[s], DOC_TILES).astype(F32)
        for q in range(copies):
            payload[q, base + slots + s : base + slots + s + 1, 2 * LANES : 3 * LANES] = jnp.full(
                (1, LANES), mark, F32
            )
    for q in range(copies):
        payload[q, base + slots : base + 2 * slots, 0:LANES] = gram[:half]
        payload[q, base + slots : base + 2 * slots, LANES : 2 * LANES] = gram[half:]
        payload[q, base + slots : base + 2 * slots, 3 * LANES :] = jnp.zeros(
            (slots, edge - 3 * LANES), F32
        )


def specs(*spaces):
    return [pl.BlockSpec(memory_space=space) for space in spaces]


def first_forward(copies, rows, cols, in_use, tiles, picked, gram, sums):
    slots, vectors, edge = picked.shape
    height = slots * vectors + 2 * slots
    return pl.pallas_call(
        functools.partial(first_forward_body, len(sums)),
        in_specs=specs(*[SMEM] * 3, *[VMEM] * (3 + len(sums))),
        out_specs=specs(VMEM, VMEM),
        out_shape=[
            jax.ShapeDtypeStruct((copies, height, edge), F32),
            jax.ShapeDtypeStruct((slots, edge), F32),
        ],
        name="first_forward",
    )(rows, cols, in_use, tiles, picked, gram, *sums)


def backward_body(
    rows, near, far, tiles, col_scale,
    dense, row_scale, low_half, high_half, gram, where, total, degree, marks, semaphores,
):
    members = near.shape[0]
    slots, edge = col_scale.shape
    vectors = dense.shape[1]
    base = slots * vectors
    tops = base + slots
    copies = [
        pltpu.make_async_copy(
            ref.at[:, tops : tops + slots, 2 * LANES : 3 * LANES], marks.at[p], semaphores.at[p]
        )
        for p, ref in enumerate((near, far))
    ]
    for copy in copies:
        copy.start()
    total[...] = jnp.zeros(total.shape, F32)
    degree[...] = jnp.ones(degree.shape, F32)
    first = jnp.zeros((slots, LANES), F32)
    second = jnp.zeros((slots, LANES), F32)
    for ref in (near, far):
        for d in range(members):
            first = first + ref[d, tops : tops + slots, 0:LANES]
            second = second + ref[d, tops : tops + slots, LANES : 2 * LANES]
    gram[0:slots, :] = first
    gram[slots : 2 * slots, :] = second
    for copy in copies:
        copy.wait()
    for p, ref in enumerate((near, far)):
        for d in range(members):
            for k in range(slots):
                row = marks[p, d, k, 0].astype(jnp.int32)
                where[(p * members + d) * slots + k] = row
                total[row] += ref[d, k * vectors : (k + 1) * vectors, :]
                degree[row] += ref[d, base + k : base + k + 1, :]
    degree[...] = lax.rsqrt(degree[...])
    for r in range(DOC_TILES):
        dense[r] = total[r] * degree[r]
    for s in range(slots):
        row = rows[s]
        scale = degree[row]
        row_scale[s : s + 1, :] = scale
        out = nn(split2(dense[row] * scale), tiles[s])
        product = (out[:vectors] + out[vectors:]) * col_scale[s : s + 1, :]
        if s < slots // 2:
            low_half[s * vectors : (s + 1) * vectors, :] = product
        else:
            t = s - slots // 2
            high_half[t * vectors : (t + 1) * vectors, :] = product


def backward(rows, near, far, tiles, col_scale):
    members = near.shape[0]
    slots, edge = col_scale.shape
    vectors = (near.shape[1] - 2 * slots) // slots
    half = jax.ShapeDtypeStruct((slots // 2 * vectors, edge), F32)
    return pl.pallas_call(
        backward_body,
        in_specs=specs(SMEM, *[VMEM] * 4),
        out_specs=specs(*[VMEM] * 5, SMEM),
        out_shape=[
            jax.ShapeDtypeStruct((DOC_TILES, vectors, edge), F32),
            jax.ShapeDtypeStruct((slots, edge), F32),
            half,
            half,
            jax.ShapeDtypeStruct((vectors, LANES), F32),
            jax.ShapeDtypeStruct((2 * members * slots,), jnp.int32),
        ],
        scratch_shapes=[
            pltpu.VMEM((DOC_TILES + 1, vectors, edge), F32),
            pltpu.VMEM((DOC_TILES + 1, 1, edge), F32),
            pltpu.SMEM((2, members, slots, LANES), F32),
            pltpu.SemaphoreType.DMA((2,)),
        ],
        name="backward",
    )(rows, near, far, tiles, col_scale)


def second_forward_body(groups, share, *refs):
    cols, place = refs[:2]
    tiles, col_scale, row_scale = refs[2:5]
    sums = refs[5 : 5 + groups]
    halves = refs[5 + groups : 5 + 3 * groups]
    payload, mine, total, marks, semaphores = refs[5 + 3 * groups :]
    slots, edge = col_scale.shape
    vectors = mine.shape[1]
    copies = [
        pltpu.make_async_copy(ref.at[:, edge : edge + LANES], marks.at[d], semaphores.at[d])
        for d, ref in enumerate(sums)
    ]
    for copy in copies:
        copy.start()
    total[...] = jnp.zeros(total.shape, F32)
    for copy in copies:
        copy.wait()
    for d in range(groups):
        for k in range(slots):
            mark = marks[d, k, 0].astype(jnp.int32)
            column = jnp.where(mark < 0, TERM_TILES, mark)
            part = halves[2 * d + k // (slots // 2)]
            t = k % (slots // 2)
            total[column] += part[t * vectors : (t + 1) * vectors, :]
    for s in range(slots):
        out = nt(split2(total[cols[s]] * col_scale[s : s + 1, :]), tiles[s])
        product = (out[:vectors] + out[vectors:]) * row_scale[s : s + 1, :]
        for q in range(payload.shape[0]):
            payload[q, s * vectors : (s + 1) * vectors, :] = product
    for t in range(share):
        mine[t] = total[place[0] * share + t]


def second_forward(copies, share, cols, place, tiles, col_scale, row_scale, sums, halves):
    slots, edge = col_scale.shape
    vectors = halves[0].shape[0] // (slots // 2)
    groups = len(sums)
    return pl.pallas_call(
        functools.partial(second_forward_body, groups, share),
        in_specs=specs(SMEM, SMEM, *[VMEM] * (3 + 3 * groups)),
        out_specs=specs(VMEM, VMEM),
        out_shape=[
            jax.ShapeDtypeStruct((copies, slots * vectors, edge), F32),
            jax.ShapeDtypeStruct((share, vectors, edge), F32),
        ],
        scratch_shapes=[
            pltpu.VMEM((TERM_TILES + 1, vectors, edge), F32),
            pltpu.SMEM((groups, slots, LANES), F32),
            pltpu.SemaphoreType.DMA((groups,)),
        ],
        name="second_forward",
    )(cols, place, tiles, col_scale, row_scale, *sums, *halves)


def document_gram_body(share, where, place, near, far, dense, gram, first, second, total):
    members = near.shape[0]
    _, vectors, edge = dense.shape
    slots = near.shape[1] // vectors
    total[...] = jnp.zeros(total.shape, F32)
    for p, ref in enumerate((near, far)):
        for d in range(members):
            for k in range(slots):
                row = where[(p * members + d) * slots + k]
                total[row] += ref[d, k * vectors : (k + 1) * vectors, :]
    out = jnp.zeros((6 * vectors, 6 * vectors), F32)
    for r in range(DOC_TILES):
        pieces = split3(jnp.concatenate([dense[r], total[r]], axis=0))
        out = out + nt(pieces, pieces)
    gram[...] = pad_lanes(fold3(out, 2 * vectors))
    for t in range(share):
        first[t] = dense[place[0] * share + t]
        second[t] = total[place[0] * share + t]


def document_gram(share, where, place, near, far, dense):
    _, vectors, edge = dense.shape
    piece = jax.ShapeDtypeStruct((share, vectors, edge), F32)
    return pl.pallas_call(
        functools.partial(document_gram_body, share),
        in_specs=specs(SMEM, SMEM, *[VMEM] * 3),
        out_specs=specs(*[VMEM] * 3),
        out_shape=[jax.ShapeDtypeStruct((2 * vectors, LANES), F32), piece, piece],
        scratch_shapes=[pltpu.VMEM((DOC_TILES + 1, vectors, edge), F32)],
        name="document_gram",
    )(where, place, near, far, dense)


def factorize(gram):
    edge = gram.shape[0]
    down = lax.broadcasted_iota(jnp.int32, (edge, edge), 0)
    across = lax.broadcasted_iota(jnp.int32, (edge, edge), 1)
    unit = jnp.where(down == across, 1.0, 0.0)
    work = jnp.concatenate([gram, unit], axis=1)
    index = lax.broadcasted_iota(jnp.int32, (edge, 2 * edge), 0)
    for k in range(edge):
        inverse = lax.rsqrt(work[k : k + 1, k : k + 1])
        pivot = work[k : k + 1, :] * inverse
        column = work[:, k : k + 1] * inverse
        work = jnp.where(
            index > k, work - column * pivot, jnp.where(index == k, pivot, work)
        )
    upper = jnp.where(down <= across, work[:, :edge], 0.0)
    lower = lax.dot_general(
        upper, unit, (((0,), (0,)), ((), ())), precision=HIGHEST, preferred_element_type=F32
    )
    return lower, upper, work[:, edge:]


def combine(factor, data):
    rows = factor.shape[0]
    out = nn(jnp.concatenate([split3(factor)] * 3, axis=1), split3(data))
    return out[:rows] + out[rows : 2 * rows] + out[2 * rows :]


def finish_body(groups, n_docs, n_terms, *refs):
    grams = refs[:groups]
    start_gram_ref, first, second, right_part, start = refs[groups : groups + 5]
    left_out, right_out, coefficients = refs[groups + 5 :]
    vectors = start.shape[0]
    edge = first.shape[2]
    gram = grams[0][...]
    for ref in grams[1:]:
        gram = gram + ref[...]
    low = gram[:vectors, :vectors]
    cross = gram[vectors:, :vectors]
    turned = gram[:vectors, vectors : 2 * vectors]
    high = gram[vectors:, vectors : 2 * vectors]
    mm = functools.partial(nn, precision=HIGHEST)
    mt = functools.partial(nt, precision=HIGHEST)
    _, _, inverse_zero = factorize(start_gram_ref[:, :vectors] / n_terms)
    lower_one, upper_one, inverse = factorize(mt(mm(inverse_zero, low / n_docs), inverse_zero))
    both = mm(inverse, inverse_zero)
    projection_one = upper_one * (n_docs / n_terms)
    sym = (cross + turned) * (0.5 / n_terms)
    lower_two, upper_two, inverse_two = factorize(
        mt(mm(both, sym), both) - mt(projection_one, projection_one)
    )
    projection_two = upper_two * (n_terms / n_docs)
    back = mm(projection_one, inverse_zero)
    right_factor = jnp.concatenate([mm(inverse_two, both), -mm(inverse_two, back)], axis=1)
    main = right_factor[:, :vectors]
    side = right_factor[:, vectors:] - mm(projection_two, both)
    main_high = mm(main, high) + mm(side, turned)
    main_low = mm(main, cross) + mm(side, low)
    lower_three, _, inverse_three = factorize(
        (mt(main_high, main) + mt(main_low, side)) / n_docs
    )
    left_factor = jnp.concatenate([mm(inverse_three, main), mm(inverse_three, side)], axis=1)
    for i, value in enumerate((lower_one, projection_one, lower_two, projection_two, lower_three)):
        coefficients[i] = value
    for t in range(right_part.shape[0]):
        data = jnp.concatenate([right_part[t], start[:, t * edge : (t + 1) * edge]], axis=0)
        right_out[:, t * edge : (t + 1) * edge] = combine(right_factor, data)
    for t in range(first.shape[0]):
        data = jnp.concatenate([second[t], first[t]], axis=0)
        left_out[:, t * edge : (t + 1) * edge] = combine(left_factor, data)


def finish(n_docs, n_terms, grams, gram_zero, first, second, right_part, start):
    vectors = start.shape[0]
    edge = first.shape[2]
    return pl.pallas_call(
        functools.partial(finish_body, len(grams), n_docs, n_terms),
        in_specs=specs(*[VMEM] * (len(grams) + 5)),
        out_specs=specs(*[VMEM] * 3),
        out_shape=[
            jax.ShapeDtypeStruct((vectors, first.shape[0] * edge), F32),
            jax.ShapeDtypeStruct((vectors, right_part.shape[0] * edge), F32),
            jax.ShapeDtypeStruct((5, vectors, vectors), F32),
        ],
        name="finish",
    )(*grams, gram_zero, first, second, right_part, start)


def shift(value, axis, step):
    size = lax.axis_size(axis)
    return lax.ppermute(value, axis, [(i, (i + step) % size) for i in range(size)])


def from_all(value, axis):
    return [value] + [shift(value, axis, k) for k in range(1, lax.axis_size(axis))]


def around(low, high, axis):
    size = lax.axis_size(axis)
    lows, highs = {0: low}, {0: high}
    ahead, behind = (low, high), (low, high)
    for k in range(1, size // 2 + 1):
        if 2 * k < size:
            ahead = (shift(ahead[0], axis, 1), shift(ahead[1], axis, 1))
            behind = (shift(behind[0], axis, -1), shift(behind[1], axis, -1))
            lows[k], highs[k] = ahead
            lows[size - k], highs[size - k] = behind
        else:
            lows[k] = shift(ahead[0], axis, 1)
            highs[k] = shift(behind[1], axis, -1)
    return [half for k in range(size) for half in (lows[k], highs[k])]


def term_gather(payload):
    size = lax.axis_size("term")
    near = lax.all_to_all(
        payload, "term", 0, 0,
        axis_index_groups=[list(range(0, size, 2)), list(range(1, size, 2))],
    )
    far = lax.ppermute(near, "term", [(i, i ^ 1) for i in range(size)])
    return near, far


def on_device(tiles, tile_rows, tile_cols, counts, start):
    tiles = tiles[0, 0]
    rows = tile_rows[0, 0]
    cols = tile_cols[0, 0]
    in_use = counts[0]
    doc_groups = lax.axis_size("doc")
    term_groups = lax.axis_size("term")
    edge = tiles.shape[1]
    n_docs = DOC_TILES * edge * doc_groups
    n_terms = TERM_TILES * edge * term_groups
    members = term_groups // 2
    row_share = DOC_TILES // term_groups
    col_share = TERM_TILES // doc_groups
    doc_place = lax.axis_index("doc").reshape(1)
    term_place = lax.axis_index("term").reshape(1)
    sums, picked = column_sums(tiles, start, cols, in_use)
    all_sums = from_all(sums, "doc")
    gram_zero = start_gram(start)
    payload, col_scale = first_forward(
        members, rows, cols, in_use, tiles, picked, gram_zero, all_sums
    )
    near, far = term_gather(payload)
    dense, row_scale, low_half, high_half, gram_zero, where = backward(
        rows, near, far, tiles, col_scale
    )
    halves = around(low_half, high_half, "doc")
    payload, right_part = second_forward(
        members, col_share, cols, doc_place, tiles, col_scale, row_scale, all_sums, halves
    )
    near, far = term_gather(payload)
    gram, first, second = document_gram(row_share, where, term_place, near, far, dense)
    mine = lax.dynamic_slice_in_dim(
        start, lax.axis_index("doc") * (col_share * edge), col_share * edge, 1
    )
    return finish(
        n_docs, n_terms, from_all(gram, "doc"), gram_zero, first, second, right_part, mine
    )


def solution(mesh):
    in_specs = (
        P("doc", "term", None, None, None),
        P("doc", "term", None),
        P("doc", "term", None),
        P("doc", "term"),
        P(None, "term"),
    )
    out_specs = (P(None, ("doc", "term")), P(None, ("term", "doc")), P())
    return jax.shard_map(
        on_device, mesh=mesh, in_specs=in_specs, out_specs=out_specs, check_vma=False
    )
```

```python
import functools

import jax
import jax.numpy as jnp
from jax import lax
from jax.experimental import pallas as pl
from jax.experimental.pallas import tpu as pltpu
from jax.sharding import PartitionSpec as P


TERM_TILES = 64
DOC_TILES = 32
LANES = 128
F32 = jnp.float32
BF16 = jnp.bfloat16
HIGHEST = lax.Precision.HIGHEST
HBM = pltpu.MemorySpace.HBM
VMEM = pltpu.MemorySpace.VMEM
SMEM = pltpu.MemorySpace.SMEM
SMALL = pltpu.CompilerParams(vmem_limit_bytes=8 * 1024 * 1024)


def specs(*spaces):
    return [pl.BlockSpec(memory_space=space) for space in spaces]


def inside(values, space=VMEM):
    return [pltpu.with_memory_space_constraint(value, space) for value in values]


def nn(a, b, precision=None):
    return lax.dot_general(
        a, b, (((1,), (0,)), ((), ())), precision=precision, preferred_element_type=F32
    )


def nt(a, b, precision=None):
    return lax.dot_general(
        a, b, (((1,), (1,)), ((), ())), precision=precision, preferred_element_type=F32
    )


def split2(x):
    high = x.astype(BF16)
    return jnp.concatenate([high, (x - high.astype(F32)).astype(BF16)], axis=0)


def split3(x):
    high = x.astype(BF16)
    rest = x - high.astype(F32)
    middle = rest.astype(BF16)
    low = (rest - middle.astype(F32)).astype(BF16)
    return jnp.concatenate([high, middle, low], axis=0)


def fold3(gram, left, right):
    rows = gram[:left] + gram[left : 2 * left] + gram[2 * left :]
    return rows[:, :right] + rows[:, right : 2 * right] + rows[:, 2 * right :]


def pad_lanes(x):
    return jnp.concatenate([x, jnp.zeros((x.shape[0], LANES - x.shape[1]), F32)], axis=1)


def column_sums_body(
    cols_in, in_use, tiles, start, kept, sums, picked, cols, semaphores, scalar_semaphore
):
    slots, edge, _ = kept.shape
    scalars = pltpu.make_async_copy(cols_in, cols, scalar_semaphore)
    scalars.start()
    copies = [
        pltpu.make_async_copy(tiles.at[s], kept.at[s], semaphores.at[0, s]) for s in range(slots)
    ]
    for copy in copies:
        copy.start()
    scalars.wait()
    blocks = []
    for s in range(slots):
        place = pl.multiple_of(cols[s] * edge, edge)
        block = start.at[:, pl.ds(place, edge)]
        blocks.append(pltpu.make_async_copy(block, picked.at[s], semaphores.at[1, s]))
        blocks[s].start()
    ones = jnp.ones((16, edge), BF16)
    for s in range(slots):
        live = s < in_use[0]
        mark = jnp.where(live, cols[s], -1).astype(F32)
        copies[s].wait()
        sums[s : s + 1, 0:edge] = jnp.where(live, nn(ones, kept[s])[0:1], 0.0)
        sums[s : s + 1, edge : edge + LANES] = jnp.full((1, LANES), mark, F32)
    for block in blocks:
        block.wait()


def column_sums(tiles, start, cols, in_use):
    slots, edge, _ = tiles.shape
    vectors = start.shape[0]
    return pl.pallas_call(
        column_sums_body,
        in_specs=specs(HBM, SMEM, HBM, HBM),
        out_specs=specs(VMEM, VMEM, VMEM),
        out_shape=[
            VMEM(tiles.shape, BF16),
            VMEM((slots, edge + LANES), F32),
            VMEM((slots, vectors, edge), F32),
        ],
        scratch_shapes=[
            pltpu.SMEM((slots,), jnp.int32),
            pltpu.SemaphoreType.DMA((2, slots)),
            pltpu.SemaphoreType.DMA,
        ],
        compiler_params=SMALL,
        name="column_sums",
    )(*inside([cols], HBM), in_use, *inside([tiles, start], HBM))


def first_forward_body(groups, *refs):
    rows, cols, in_use = refs[:3]
    tiles, picked = refs[3:5]
    sums = refs[5 : 5 + groups]
    low, high, whole, col_scale = refs[5 + groups :]
    slots, vectors, edge = picked.shape
    half = slots // 2
    base = half * vectors
    values = [r[:, 0:edge] for r in sums]
    marks = [r[:, edge : edge + LANES] for r in sums]
    for s in range(slots):
        column = cols[s].astype(F32)
        degree = jnp.ones((1, edge), F32)
        for value, mark in zip(values, marks):
            same = jnp.where(mark == column, 1.0, 0.0)
            same = jnp.concatenate([same] * (edge // LANES), axis=1)
            degree = degree + jnp.sum(same * value, axis=0, keepdims=True)
        scale = lax.rsqrt(degree)
        col_scale[s : s + 1, :] = scale
        left = jnp.concatenate(
            [split2(picked[s] * scale), jnp.ones((vectors, edge), BF16)], axis=0
        )
        out = nt(left, tiles[s])
        t = s % half
        product = out[:vectors] + out[vectors : 2 * vectors]
        row_sum = out[2 * vectors : 2 * vectors + 1]
        mark = jnp.full((1, edge), jnp.where(s < in_use[0], rows[s], DOC_TILES).astype(F32), F32)
        (low, high)[s // half][t * vectors : (t + 1) * vectors, :] = product
        low[base + s : base + s + 1, :] = row_sum
        high[base + s : base + s + 1, :] = mark
        top = s // half * (base + slots) + t * vectors
        whole[top : top + vectors, :] = product
        whole[base + s : base + s + 1, :] = row_sum
        whole[2 * base + slots + s : 2 * base + slots + s + 1, :] = mark


def first_forward(rows, cols, in_use, tiles, picked, sums):
    slots, vectors, edge = picked.shape
    height = slots // 2 * vectors + slots
    payload = VMEM((height, edge), F32)
    return pl.pallas_call(
        functools.partial(first_forward_body, len(sums)),
        in_specs=specs(*[SMEM] * 3, *[VMEM] * (2 + len(sums))),
        out_specs=specs(*[VMEM] * 4),
        out_shape=[payload, payload, VMEM((2 * height, edge), F32), VMEM((slots, edge), F32)],
        compiler_params=SMALL,
        name="first_forward",
    )(rows, cols, in_use, *inside([tiles, picked, *sums]))


def backward_body(offsets, *refs):
    members = len(offsets) // 2
    rows = refs[0]
    halves = refs[1 : 1 + 2 * members]
    tiles, col_scale = refs[1 + 2 * members : 3 + 2 * members]
    dense, row_scale, low_half, high_half, where = refs[3 + 2 * members : 8 + 2 * members]
    total, degree, marks, semaphores = refs[8 + 2 * members :]
    slots, _ = col_scale.shape
    vectors = dense.shape[1]
    half = slots // 2
    base = half * vectors
    copies = [
        pltpu.make_async_copy(
            halves[2 * p + 1].at[
                offsets[2 * p + 1] + base : offsets[2 * p + 1] + base + slots, 0:LANES
            ],
            marks.at[p],
            semaphores.at[p],
        )
        for p in range(members)
    ]
    for copy in copies:
        copy.start()
    total[...] = jnp.zeros(total.shape, F32)
    degree[...] = jnp.ones(degree.shape, F32)
    for copy in copies:
        copy.wait()
    for p in range(members):
        for k in range(slots):
            row = marks[p, k, 0].astype(jnp.int32)
            where[p * slots + k] = row
            which = 2 * p + k // half
            top = offsets[which] + k % half * vectors
            total[row] += halves[which][top : top + vectors, :]
            top = offsets[2 * p] + base + k
            degree[row] += halves[2 * p][top : top + 1, :]
    degree[...] = lax.rsqrt(degree[...])
    for r in range(DOC_TILES):
        dense[r] = total[r] * degree[r]
    for s in range(slots):
        row = rows[s]
        scale = degree[row]
        row_scale[s : s + 1, :] = scale
        out = nn(split2(dense[row] * scale), tiles[s])
        product = (out[:vectors] + out[vectors:]) * col_scale[s : s + 1, :]
        t = s % half
        (low_half, high_half)[s // half][t * vectors : (t + 1) * vectors, :] = product


def backward(rows, gathered, tiles, col_scale):
    halves, offsets = gathered
    members = len(halves) // 2
    slots, edge = col_scale.shape
    vectors = (halves[0].shape[0] - slots) // (slots // 2)
    half = VMEM((slots // 2 * vectors, edge), F32)
    return pl.pallas_call(
        functools.partial(backward_body, offsets),
        in_specs=specs(SMEM, *[VMEM] * (2 * members + 2)),
        out_specs=specs(*[VMEM] * 4, SMEM),
        out_shape=[
            VMEM((DOC_TILES, vectors, edge), F32),
            VMEM((slots, edge), F32),
            half,
            half,
            jax.ShapeDtypeStruct((members * slots,), jnp.int32),
        ],
        scratch_shapes=[
            pltpu.VMEM((DOC_TILES + 1, vectors, edge), F32),
            pltpu.VMEM((DOC_TILES + 1, 1, edge), F32),
            pltpu.SMEM((members, slots, LANES), F32),
            pltpu.SemaphoreType.DMA((members,)),
        ],
        compiler_params=SMALL,
        name="backward",
    )(rows, *inside([*halves, tiles, col_scale]))


def second_forward_body(groups, share, *refs):
    cols = refs[0]
    tiles, col_scale, row_scale = refs[1:4]
    grams = refs[4 : 4 + groups]
    sums = refs[4 + groups : 4 + 2 * groups]
    halves = refs[4 + 2 * groups : 4 + 4 * groups]
    low, high, whole, mine, total, marks, semaphores = refs[4 + 4 * groups :]
    slots, edge = col_scale.shape
    vectors = mine.shape[1]
    half = slots // 2
    place = lax.axis_index("doc") * share
    copies = [
        pltpu.make_async_copy(ref.at[:, edge : edge + LANES], marks.at[d], semaphores.at[d])
        for d, ref in enumerate(sums)
    ]
    for copy in copies:
        copy.start()
    total[...] = jnp.zeros(total.shape, F32)
    for copy in copies:
        copy.wait()
    for d in range(groups):
        for k in range(slots):
            mark = marks[d, k, 0].astype(jnp.int32)
            column = jnp.where(mark < 0, TERM_TILES, mark)
            t = k % half
            total[column] += halves[2 * d + k // half][t * vectors : (t + 1) * vectors, :]
    for s in range(slots):
        out = nt(split2(total[cols[s]] * col_scale[s : s + 1, :]), tiles[s])
        product = (out[:vectors] + out[vectors:]) * row_scale[s : s + 1, :]
        t = s % half
        (low, high)[s // half][t * vectors : (t + 1) * vectors, :] = product
        whole[s * vectors : (s + 1) * vectors, :] = product
    gram = grams[0][...]
    for ref in grams[1:]:
        gram = gram + ref[...]
    extra = jnp.concatenate(
        [gram[:slots], gram[slots:], jnp.zeros((slots, edge - 2 * LANES), F32)], axis=1
    )
    high[half * vectors :, :] = extra
    whole[slots * vectors :, :] = extra
    for t in range(share):
        mine[t] = total[place + t]


def second_forward(share, cols, tiles, col_scale, row_scale, grams, sums, halves):
    slots, edge = col_scale.shape
    vectors = halves[0].shape[0] // (slots // 2)
    groups = len(sums)
    base = slots // 2 * vectors
    return pl.pallas_call(
        functools.partial(second_forward_body, groups, share),
        in_specs=specs(SMEM, *[VMEM] * (3 + 4 * groups)),
        out_specs=specs(*[VMEM] * 4),
        out_shape=[
            VMEM((base, edge), F32),
            VMEM((base + slots, edge), F32),
            VMEM((2 * base + slots, edge), F32),
            VMEM((share, vectors, edge), F32),
        ],
        scratch_shapes=[
            pltpu.VMEM((TERM_TILES + 1, vectors, edge), F32),
            pltpu.SMEM((groups, slots, LANES), F32),
            pltpu.SemaphoreType.DMA((groups,)),
        ],
        compiler_params=SMALL,
        name="second_forward",
    )(cols, *inside([tiles, col_scale, row_scale, *grams, *sums, *halves]))


def low_gram_body(dense, start, gram, own, semaphore):
    rows, vectors, edge = dense.shape
    count = own.shape[1]
    place = pl.multiple_of(lax.axis_index("doc") * count, count)
    copy = pltpu.make_async_copy(start.at[:, pl.ds(place, count)], own, semaphore)
    copy.start()
    low = jnp.zeros((3 * vectors, 3 * vectors), F32)
    for r in range(rows):
        pieces = split3(dense[r])
        low = low + nt(pieces, pieces)
    copy.wait()
    first = jnp.zeros((3 * vectors, 3 * vectors), F32)
    for c in range(0, count, edge):
        pieces = split3(own[:, c : c + edge])
        first = first + nt(pieces, pieces)
    gram[...] = pad_lanes(
        jnp.concatenate([fold3(low, vectors, vectors), fold3(first, vectors, vectors)], axis=1)
    )


def low_gram(count, dense, start):
    vectors = dense.shape[1]
    return pl.pallas_call(
        low_gram_body,
        in_specs=specs(VMEM, HBM),
        out_specs=specs(VMEM, VMEM),
        out_shape=[VMEM((vectors, LANES), F32), VMEM((vectors, count), F32)],
        scratch_shapes=[pltpu.SemaphoreType.DMA],
        compiler_params=SMALL,
        name="low_gram",
    )(*inside([dense]), *inside([start], HBM))


def high_gram_body(share, offsets, *refs):
    members = len(offsets) // 2
    where = refs[0]
    halves = refs[1 : 1 + 2 * members]
    dense, gram, start_part, first, second, total = refs[1 + 2 * members :]
    rows, vectors, _ = dense.shape
    half = halves[0].shape[0] // vectors
    slots = 2 * half
    base = half * vectors
    place = lax.axis_index("term") * share
    for k in range(2):
        part = jnp.zeros((slots, LANES), F32)
        for p in range(members):
            top = offsets[2 * p + 1] + base
            part = part + halves[2 * p + 1][top : top + slots, k * LANES : (k + 1) * LANES]
        start_part[k * slots : (k + 1) * slots, :] = part
    total[...] = jnp.zeros(total.shape, F32)
    for p in range(members):
        for k in range(slots):
            which = 2 * p + k // half
            top = offsets[which] + k % half * vectors
            total[where[p * slots + k]] += halves[which][top : top + vectors, :]
    out = jnp.zeros((3 * vectors, 6 * vectors), F32)
    for r in range(rows):
        data = total[r]
        out = out + nt(split3(data), split3(jnp.concatenate([dense[r], data], axis=0)))
    gram[...] = pad_lanes(fold3(out, vectors, 2 * vectors))
    for t in range(share):
        first[t] = dense[place + t]
        second[t] = total[place + t]


def high_gram(share, where, gathered, dense):
    halves, offsets = gathered
    _, vectors, edge = dense.shape
    members = len(halves) // 2
    piece = VMEM((share, vectors, edge), F32)
    return pl.pallas_call(
        functools.partial(high_gram_body, share, offsets),
        in_specs=specs(SMEM, *[VMEM] * (2 * members + 1)),
        out_specs=specs(*[VMEM] * 4),
        out_shape=[VMEM((vectors, LANES), F32), VMEM((vectors, LANES), F32), piece, piece],
        scratch_shapes=[pltpu.VMEM((DOC_TILES + 1, vectors, edge), F32)],
        compiler_params=SMALL,
        name="high_gram",
    )(where, *inside([*halves, dense]))


def factorize(gram):
    edge = gram.shape[0]
    down = lax.broadcasted_iota(jnp.int32, (edge, edge), 0)
    across = lax.broadcasted_iota(jnp.int32, (edge, edge), 1)
    index = lax.broadcasted_iota(jnp.int32, (edge, 2 * edge), 0)
    work = jnp.concatenate([gram, jnp.where(down == across, 1.0, 0.0)], axis=1)
    columns = [jnp.broadcast_to(gram[:, j : j + 1], (edge, 2 * edge)) for j in range(edge)]
    lower = jnp.zeros((edge, edge), F32)
    for k in range(edge):
        inverse = lax.rsqrt(columns[k][k : k + 1, :])
        column = columns[k] * inverse
        pivot = work[k : k + 1, :] * inverse
        work = jnp.where(index > k, work - column * pivot, jnp.where(index == k, pivot, work))
        lower = jnp.where((across == k) & (down >= k), column[:, :edge], lower)
        for j in range(k + 1, edge):
            columns[j] = columns[j] - column * column[j : j + 1, :]
    return lower, jnp.where(down <= across, work[:, :edge], 0.0), work[:, edge:]


def combine(factor, data):
    rows = factor.shape[0]
    out = nn(jnp.concatenate([split3(factor)] * 3, axis=1), split3(data))
    return out[:rows] + out[rows : 2 * rows] + out[2 * rows :]


MM = functools.partial(nn, precision=HIGHEST)
MT = functools.partial(nt, precision=HIGHEST)


def prepare_body(groups, n_docs, n_terms, *refs):
    start_gram_ref = refs[0]
    grams = refs[1 : 1 + groups]
    (out,) = refs[1 + groups :]
    vectors = out.shape[1]
    low = grams[0][...]
    for ref in grams[1:]:
        low = low + ref[...]
    low = low[:, :vectors]
    _, _, inverse_zero = factorize(start_gram_ref[:, vectors : 2 * vectors] / n_terms)
    lower_one, upper_one, inverse = factorize(MT(MM(inverse_zero, low / n_docs), inverse_zero))
    projection = upper_one * (n_docs / n_terms)
    values = (
        low,
        lower_one,
        projection,
        MT(projection, projection),
        MM(inverse, inverse_zero),
        MM(projection, inverse_zero),
    )
    for i, value in enumerate(values):
        out[i] = pad_lanes(value)


def prepare(n_docs, n_terms, gram_zero, grams):
    vectors = gram_zero.shape[0]
    return pl.pallas_call(
        functools.partial(prepare_body, len(grams), n_docs, n_terms),
        in_specs=specs(*[VMEM] * (1 + len(grams))),
        out_specs=pl.BlockSpec(memory_space=VMEM),
        out_shape=VMEM((6, vectors, LANES), F32),
        compiler_params=SMALL,
        name="prepare",
    )(*inside([gram_zero, *grams]))


def finish_body(groups, n_docs, n_terms, *refs):
    grams = refs[:groups]
    ready, first, second, right_part, own = refs[groups : groups + 5]
    left_out, right_out, coefficients = refs[groups + 5 :]
    share, vectors, edge = right_part.shape
    gram = grams[0][...]
    for ref in grams[1:]:
        gram = gram + ref[...]
    cross = gram[:, :vectors]
    high = gram[:, vectors : 2 * vectors]
    low, lower_one, projection_one, square, both, back = [
        ready[i][:, :vectors] for i in range(6)
    ]
    lower_two, upper_two, inverse_two = factorize(MT(MM(both, cross / n_terms), both) - square)
    projection_two = upper_two * (n_terms / n_docs)
    main = MM(inverse_two, both)
    minus = MM(inverse_two, back)
    side = minus + MM(projection_two, both)
    right_factor = jnp.concatenate([main, -minus], axis=1)
    main_high = MM(main, high) - MT(side, cross)
    main_low = MM(main, cross) - MM(side, low)
    lower_three, _, inverse_three = factorize(
        (MT(main_high, main) - MT(main_low, side)) / n_docs
    )
    left_factor = jnp.concatenate([MM(inverse_three, main), -MM(inverse_three, side)], axis=1)
    for i, value in enumerate((lower_one, projection_one, lower_two, projection_two, lower_three)):
        coefficients[i] = value
    for t in range(share):
        data = jnp.concatenate([right_part[t], own[:, t * edge : (t + 1) * edge]], axis=0)
        right_out[:, t * edge : (t + 1) * edge] = combine(right_factor, data)
    for t in range(first.shape[0]):
        data = jnp.concatenate([second[t], first[t]], axis=0)
        left_out[:, t * edge : (t + 1) * edge] = combine(left_factor, data)


def finish(n_docs, n_terms, grams, ready, first, second, right_part, own):
    share, vectors, edge = right_part.shape
    return pl.pallas_call(
        functools.partial(finish_body, len(grams), n_docs, n_terms),
        in_specs=specs(*[VMEM] * (len(grams) + 5)),
        out_specs=specs(*[VMEM] * 3),
        out_shape=[
            jax.ShapeDtypeStruct((vectors, first.shape[0] * edge), F32),
            jax.ShapeDtypeStruct((vectors, share * edge), F32),
            jax.ShapeDtypeStruct((5, vectors, vectors), F32),
        ],
        compiler_params=SMALL,
        name="finish",
    )(*inside([*grams, ready, first, second, right_part, own]))


def shift(value, axis, step):
    size = lax.axis_size(axis)
    return lax.ppermute(value, axis, [(i, (i + step) % size) for i in range(size)])


def hop(value, mask):
    return lax.ppermute(value, "term", [(i, i ^ mask) for i in range(lax.axis_size("term"))])


def from_all(value, axis):
    return [value] + [shift(value, axis, k) for k in range(1, lax.axis_size(axis))]


def around(low, high, axis):
    size = lax.axis_size(axis)
    lows, highs = {0: low}, {0: high}
    ahead, behind = (low, high), (low, high)
    for k in range(1, size // 2 + 1):
        if 2 * k < size:
            ahead = (shift(ahead[0], axis, 1), shift(ahead[1], axis, 1))
            behind = (shift(behind[0], axis, -1), shift(behind[1], axis, -1))
            lows[k], highs[k] = ahead
            lows[size - k], highs[size - k] = behind
        else:
            lows[k] = shift(ahead[0], axis, 1)
            highs[k] = shift(behind[1], axis, -1)
    return [half for k in range(size) for half in (lows[k], highs[k])]


STEPS = (
    ("low_x", "low", 2),
    ("high_y", "high", 4),
    ("high_x", "high", 2),
    ("low_y", "low", 4),
    ("whole_p", "whole", 1),
    ("low_d", "low_x", 4),
    ("high_d", "high_y", 2),
    ("low_x_p", "low_x", 1),
    ("high_y_p", "high_y", 1),
    ("high_x_p", "high_x", 1),
    ("low_y_p", "low_y", 1),
    ("high_d_p", "high_d", 1),
    ("low_d_p", "low_d", 1),
)


def term_gather(low, high, whole):
    if lax.axis_size("term") != 8:
        halves = [h for pair in zip(from_all(low, "term"), from_all(high, "term")) for h in pair]
        return halves, (0,) * len(halves)
    held = {"low": low, "high": high, "whole": whole}
    for name, source, mask in STEPS:
        held[name] = hop(held[source], mask)
    held["low_p"] = held["high_p"] = held["whole_p"]
    halves, offsets = [], []
    for end in ("", "_x", "_y", "_d", "_p", "_x_p", "_y_p", "_d_p"):
        halves += [held["low" + end], held["high" + end]]
        offsets += [0, low.shape[0] if end == "_p" else 0]
    return halves, tuple(offsets)


def after(values, first):
    return lax.optimization_barrier((values, first))[0]


def on_device(tiles, tile_rows, tile_cols, counts, start):
    return program(tiles[0, 0], tile_rows[0, 0], tile_cols[0, 0], counts[0], start)


def program(tiles, rows, cols, in_use, start):
    doc_groups = lax.axis_size("doc")
    term_groups = lax.axis_size("term")
    edge = tiles.shape[1]
    n_docs = DOC_TILES * edge * doc_groups
    n_terms = TERM_TILES * edge * term_groups
    row_share = DOC_TILES // term_groups
    col_share = TERM_TILES // doc_groups
    tiles, sums, picked = column_sums(tiles, start, cols, in_use)
    all_sums = from_all(sums, "doc")
    low, high, whole, col_scale = first_forward(rows, cols, in_use, tiles, picked, all_sums)
    dense, row_scale, low, high, where = backward(
        rows, term_gather(low, high, whole), tiles, col_scale
    )
    halves = around(low, high, "doc")
    low_part, own = low_gram(col_share * edge, after(dense, halves[2]), start)
    low_grams = from_all(low_part, "doc")
    halves, low_grams = lax.optimization_barrier((halves, low_grams))
    low, high, whole, right_part = second_forward(
        col_share, cols, tiles, col_scale, row_scale, low_grams, all_sums, halves
    )
    gram, gram_zero, first, second = high_gram(
        row_share, where, term_gather(low, high, whole), dense
    )
    ready = prepare(n_docs, n_terms, *after((gram_zero, low_grams), gram))
    return finish(n_docs, n_terms, from_all(gram, "doc"), ready, first, second, right_part, own)


def solution(mesh):
    in_specs = (
        P("doc", "term", None, None, None),
        P("doc", "term", None),
        P("doc", "term", None),
        P("doc", "term"),
        P(None, "term"),
    )
    out_specs = (P(None, ("doc", "term")), P(None, ("term", "doc")), P())
    return jax.shard_map(
        on_device, mesh=mesh, in_specs=in_specs, out_specs=out_specs, check_vma=False
    )
```

```python
import functools

import jax
import jax.numpy as jnp
from jax import lax
from jax.experimental import pallas as pl
from jax.experimental.pallas import tpu as pltpu
from jax.sharding import PartitionSpec as P


TERM_TILES = 64
DOC_TILES = 32
LANES = 128
F32 = jnp.float32
BF16 = jnp.bfloat16
HIGHEST = lax.Precision.HIGHEST
HBM = pltpu.MemorySpace.HBM
VMEM = pltpu.MemorySpace.VMEM
SMEM = pltpu.MemorySpace.SMEM
SMALL = pltpu.CompilerParams(vmem_limit_bytes=8 * 1024 * 1024)


def specs(*spaces):
    return [pl.BlockSpec(memory_space=space) for space in spaces]


def inside(values, space=VMEM):
    return [pltpu.with_memory_space_constraint(value, space) for value in values]


def nn(a, b, precision=None):
    return lax.dot_general(
        a, b, (((1,), (0,)), ((), ())), precision=precision, preferred_element_type=F32
    )


def nt(a, b, precision=None):
    return lax.dot_general(
        a, b, (((1,), (1,)), ((), ())), precision=precision, preferred_element_type=F32
    )


def split2(x):
    high = x.astype(BF16)
    return jnp.concatenate([high, (x - high.astype(F32)).astype(BF16)], axis=0)


def split3(x):
    high = x.astype(BF16)
    rest = x - high.astype(F32)
    middle = rest.astype(BF16)
    low = (rest - middle.astype(F32)).astype(BF16)
    return jnp.concatenate([high, middle, low], axis=0)


def fold3(gram, left, right):
    rows = gram[:left] + gram[left : 2 * left] + gram[2 * left :]
    return rows[:, :right] + rows[:, right : 2 * right] + rows[:, 2 * right :]


def scalar(ref, row, lane=0):
    return ref[row : row + 1, lane : lane + 1][0, 0].astype(jnp.int32)


def pad_lanes(x):
    return jnp.concatenate([x, jnp.zeros((x.shape[0], LANES - x.shape[1]), F32)], axis=1)


def column_sums_body(
    cols_in, rows_in, in_use, tiles, start,
    kept, sums, picked, places, cols, rows, semaphores, scalar_semaphores,
):
    slots, edge, _ = kept.shape
    scalars = [
        pltpu.make_async_copy(cols_in, cols, scalar_semaphores.at[0]),
        pltpu.make_async_copy(rows_in, rows, scalar_semaphores.at[1]),
    ]
    for copy in scalars:
        copy.start()
    copies = [
        pltpu.make_async_copy(tiles.at[s], kept.at[s], semaphores.at[0, s]) for s in range(slots)
    ]
    for copy in copies:
        copy.start()
    for copy in scalars:
        copy.wait()
    blocks = []
    for s in range(slots):
        place = pl.multiple_of(cols[s] * edge, edge)
        block = start.at[:, pl.ds(place, edge)]
        blocks.append(pltpu.make_async_copy(block, picked.at[s], semaphores.at[1, s]))
        blocks[s].start()
    ones = jnp.ones((16, edge), BF16)
    for s in range(slots):
        live = s < in_use[0]
        mark = jnp.where(live, cols[s], -1).astype(F32)
        places[s : s + 1, :] = jnp.full(
            (1, LANES), jnp.where(live, rows[s], DOC_TILES).astype(F32), F32
        )
        copies[s].wait()
        sums[s : s + 1, 0:edge] = jnp.where(live, nn(ones, kept[s])[0:1], 0.0)
        sums[s : s + 1, edge : edge + LANES] = jnp.full((1, LANES), mark, F32)
    for block in blocks:
        block.wait()


def column_sums(tiles, start, cols, rows, in_use):
    slots, edge, _ = tiles.shape
    vectors = start.shape[0]
    return pl.pallas_call(
        column_sums_body,
        in_specs=specs(HBM, HBM, SMEM, HBM, HBM),
        out_specs=specs(*[VMEM] * 4),
        out_shape=[
            VMEM(tiles.shape, BF16),
            VMEM((slots, edge + LANES), F32),
            VMEM((slots, vectors, edge), F32),
            VMEM((slots, LANES), F32),
        ],
        scratch_shapes=[
            pltpu.SMEM((slots,), jnp.int32),
            pltpu.SMEM((slots,), jnp.int32),
            pltpu.SemaphoreType.DMA((2, slots)),
            pltpu.SemaphoreType.DMA((2,)),
        ],
        compiler_params=SMALL,
        name="column_sums",
    )(*inside([cols, rows], HBM), in_use, *inside([tiles, start], HBM))


def first_forward_body(groups, *refs):
    tiles, picked, places, gram = refs[:4]
    sums = refs[4 : 4 + groups]
    low, high, whole, col_scale = refs[4 + groups :]
    slots, vectors, edge = picked.shape
    half = slots // 2
    base = half * vectors
    values = [r[:, 0:edge] for r in sums]
    marks = [r[:, edge : edge + LANES] for r in sums]
    extra = jnp.concatenate(
        [places[...], gram[:slots], gram[slots:], jnp.zeros((slots, edge - 3 * LANES), F32)], axis=1
    )
    high[base:, :] = extra
    whole[2 * base + slots :, :] = extra
    for s in range(slots):
        column = marks[0][s : s + 1, :]
        degree = jnp.ones((1, edge), F32)
        for value, mark in zip(values, marks):
            same = jnp.where(mark == column, 1.0, 0.0)
            same = jnp.concatenate([same] * (edge // LANES), axis=1)
            degree = degree + jnp.sum(same * value, axis=0, keepdims=True)
        scale = lax.rsqrt(degree)
        col_scale[s : s + 1, :] = scale
        left = jnp.concatenate(
            [split2(picked[s] * scale), jnp.ones((vectors, edge), BF16)], axis=0
        )
        out = nt(left, tiles[s])
        t = s % half
        product = out[:vectors] + out[vectors : 2 * vectors]
        row_sum = out[2 * vectors : 2 * vectors + 1]
        (low, high)[s // half][t * vectors : (t + 1) * vectors, :] = product
        low[base + s : base + s + 1, :] = row_sum
        top = s // half * (base + slots) + t * vectors
        whole[top : top + vectors, :] = product
        whole[base + s : base + s + 1, :] = row_sum


def first_forward(tiles, picked, places, gram, sums):
    slots, vectors, edge = picked.shape
    height = slots // 2 * vectors + slots
    payload = VMEM((height, edge), F32)
    return pl.pallas_call(
        functools.partial(first_forward_body, len(sums)),
        in_specs=specs(*[VMEM] * (4 + len(sums))),
        out_specs=specs(*[VMEM] * 4),
        out_shape=[payload, payload, VMEM((2 * height, edge), F32), VMEM((slots, edge), F32)],
        compiler_params=SMALL,
        name="first_forward",
    )(*inside([tiles, picked, places, gram, *sums]))


def backward_body(offsets, *refs):
    members = len(offsets) // 2
    halves = refs[: 2 * members]
    tiles, col_scale = refs[2 * members : 2 + 2 * members]
    dense, row_scale, low_half, high_half, where, gram, total, degree = refs[2 + 2 * members :]
    slots, _ = col_scale.shape
    vectors = dense.shape[1]
    half = slots // 2
    base = half * vectors
    total[...] = jnp.zeros(total.shape, F32)
    degree[...] = jnp.ones(degree.shape, F32)
    for k in range(2):
        part = jnp.zeros((slots, LANES), F32)
        for p in range(members):
            top = offsets[2 * p + 1] + base
            part = part + halves[2 * p + 1][top : top + slots, (k + 1) * LANES : (k + 2) * LANES]
        gram[k * slots : (k + 1) * slots, :] = part
    mine = []
    for p in range(members):
        marks = halves[2 * p + 1]
        top = offsets[2 * p + 1] + base
        where[p * slots : (p + 1) * slots, :] = marks[top : top + slots, 0:LANES]
        for k in range(slots):
            row = scalar(marks, top + k)
            if p == 0:
                mine.append(jnp.minimum(row, DOC_TILES - 1))
            which = 2 * p + k // half
            place = offsets[which] + k % half * vectors
            total[row] += halves[which][place : place + vectors, :]
            place = offsets[2 * p] + base + k
            degree[row] += halves[2 * p][place : place + 1, :]
    degree[...] = lax.rsqrt(degree[...])
    for r in range(DOC_TILES):
        dense[r] = total[r] * degree[r]
    for s in range(slots):
        row = mine[s]
        scale = degree[row]
        row_scale[s : s + 1, :] = scale
        out = nn(split2(dense[row] * scale), tiles[s])
        product = (out[:vectors] + out[vectors:]) * col_scale[s : s + 1, :]
        t = s % half
        (low_half, high_half)[s // half][t * vectors : (t + 1) * vectors, :] = product


def backward(gathered, tiles, col_scale):
    halves, offsets = gathered
    members = len(halves) // 2
    slots, edge = col_scale.shape
    vectors = (halves[0].shape[0] - slots) // (slots // 2)
    half = VMEM((slots // 2 * vectors, edge), F32)
    return pl.pallas_call(
        functools.partial(backward_body, offsets),
        in_specs=specs(*[VMEM] * (2 * members + 2)),
        out_specs=specs(*[VMEM] * 6),
        out_shape=[
            VMEM((DOC_TILES, vectors, edge), F32),
            VMEM((slots, edge), F32),
            half,
            half,
            VMEM((members * slots, LANES), F32),
            VMEM((2 * slots, LANES), F32),
        ],
        scratch_shapes=[
            pltpu.VMEM((DOC_TILES + 1, vectors, edge), F32),
            pltpu.VMEM((DOC_TILES + 1, 1, edge), F32),
        ],
        compiler_params=SMALL,
        name="backward",
    )(*inside([*halves, tiles, col_scale]))


def second_forward_body(groups, share, *refs):
    tiles, col_scale, row_scale = refs[:3]
    sums = refs[3 : 3 + groups]
    halves = refs[3 + groups : 3 + 3 * groups]
    low, high, whole, mine, total = refs[3 + 3 * groups :]
    slots, edge = col_scale.shape
    vectors = mine.shape[1]
    half = slots // 2
    place = lax.axis_index("doc") * share
    total[...] = jnp.zeros(total.shape, F32)
    own = []
    for d in range(groups):
        for k in range(slots):
            mark = scalar(sums[d], k, edge)
            column = jnp.where(mark < 0, TERM_TILES, mark)
            if d == 0:
                own.append(column)
            t = k % half
            total[column] += halves[2 * d + k // half][t * vectors : (t + 1) * vectors, :]
    for s in range(slots):
        out = nt(split2(total[own[s]] * col_scale[s : s + 1, :]), tiles[s])
        product = (out[:vectors] + out[vectors:]) * row_scale[s : s + 1, :]
        t = s % half
        (low, high)[s // half][t * vectors : (t + 1) * vectors, :] = product
        whole[s * vectors : (s + 1) * vectors, :] = product
    for t in range(share):
        mine[t] = total[place + t]


def second_forward(share, tiles, col_scale, row_scale, sums, halves):
    slots, edge = col_scale.shape
    vectors = halves[0].shape[0] // (slots // 2)
    groups = len(sums)
    base = slots // 2 * vectors
    return pl.pallas_call(
        functools.partial(second_forward_body, groups, share),
        in_specs=specs(*[VMEM] * (3 + 3 * groups)),
        out_specs=specs(*[VMEM] * 4),
        out_shape=[
            VMEM((base, edge), F32),
            VMEM((base, edge), F32),
            VMEM((2 * base, edge), F32),
            VMEM((share, vectors, edge), F32),
        ],
        scratch_shapes=[pltpu.VMEM((TERM_TILES + 1, vectors, edge), F32)],
        compiler_params=SMALL,
        name="second_forward",
    )(*inside([tiles, col_scale, row_scale, *sums, *halves]))


def own_gram_body(start, gram, own, semaphores):
    vectors, count = own.shape
    pieces = semaphores.shape[0]
    step = count // pieces
    place = lax.axis_index("doc") * count
    copies = []
    for c in range(pieces):
        block = start.at[:, pl.ds(pl.multiple_of(place + c * step, step), step)]
        copies.append(
            pltpu.make_async_copy(block, own.at[:, c * step : (c + 1) * step], semaphores.at[c])
        )
        copies[c].start()
    total = jnp.zeros((3 * vectors, 3 * vectors), F32)
    for c in range(pieces):
        copies[c].wait()
        for t in range(c * step, (c + 1) * step, 512):
            data = split3(own[:, t : t + 512])
            total = total + nt(data, data)
    gram[...] = pad_lanes(fold3(total, vectors, vectors))


def own_gram(count, start):
    vectors = start.shape[0]
    return pl.pallas_call(
        own_gram_body,
        in_specs=specs(HBM),
        out_specs=specs(VMEM, VMEM),
        out_shape=[VMEM((vectors, LANES), F32), VMEM((vectors, count), F32)],
        scratch_shapes=[pltpu.SemaphoreType.DMA((2,))],
        compiler_params=SMALL,
        name="own_gram",
    )(*inside([start], HBM))


def low_gram_body(dense, extra, gram):
    rows, vectors, _ = dense.shape
    low = jnp.zeros((3 * vectors, 3 * vectors), F32)
    for r in range(rows):
        pieces = split3(dense[r])
        low = low + nt(pieces, pieces)
    gram[...] = pad_lanes(
        jnp.concatenate([fold3(low, vectors, vectors), extra[:, :vectors]], axis=1)
    )


def low_gram(dense, extra):
    return pl.pallas_call(
        low_gram_body,
        in_specs=specs(VMEM, VMEM),
        out_specs=pl.BlockSpec(memory_space=VMEM),
        out_shape=VMEM(extra.shape, F32),
        compiler_params=SMALL,
        name="low_gram",
    )(*inside([dense, extra]))


def high_gram_body(share, offsets, *refs):
    members = len(offsets) // 2
    where = refs[0]
    halves = refs[1 : 1 + 2 * members]
    dense, gram, first, second, total = refs[1 + 2 * members :]
    rows, vectors, _ = dense.shape
    half = halves[0].shape[0] // vectors
    slots = 2 * half
    place = lax.axis_index("term") * share
    total[...] = jnp.zeros(total.shape, F32)
    for p in range(members):
        for k in range(slots):
            which = 2 * p + k // half
            top = offsets[which] + k % half * vectors
            total[scalar(where, p * slots + k)] += halves[which][top : top + vectors, :]
    out = jnp.zeros((3 * vectors, 6 * vectors), F32)
    for r in range(rows):
        data = total[r]
        out = out + nt(split3(data), split3(jnp.concatenate([dense[r], data], axis=0)))
    gram[...] = pad_lanes(fold3(out, vectors, 2 * vectors))
    for t in range(share):
        first[t] = dense[place + t]
        second[t] = total[place + t]


def high_gram(share, where, gathered, dense):
    halves, offsets = gathered
    _, vectors, edge = dense.shape
    members = len(halves) // 2
    piece = VMEM((share, vectors, edge), F32)
    return pl.pallas_call(
        functools.partial(high_gram_body, share, offsets),
        in_specs=specs(*[VMEM] * (2 * members + 2)),
        out_specs=specs(*[VMEM] * 3),
        out_shape=[VMEM((vectors, LANES), F32), piece, piece],
        scratch_shapes=[pltpu.VMEM((DOC_TILES + 1, vectors, edge), F32)],
        compiler_params=SMALL,
        name="high_gram",
    )(*inside([where, *halves, dense]))


def factorize(gram):
    edge = gram.shape[0]
    down = lax.broadcasted_iota(jnp.int32, (edge, edge), 0)
    across = lax.broadcasted_iota(jnp.int32, (edge, edge), 1)
    index = lax.broadcasted_iota(jnp.int32, (edge, 2 * edge), 0)
    work = jnp.concatenate([gram, jnp.where(down == across, 1.0, 0.0)], axis=1)
    columns = [jnp.broadcast_to(gram[:, j : j + 1], (edge, 2 * edge)) for j in range(edge)]
    lower = jnp.zeros((edge, edge), F32)
    for k in range(edge):
        inverse = lax.rsqrt(columns[k][k : k + 1, :])
        column = columns[k] * inverse
        pivot = work[k : k + 1, :] * inverse
        work = jnp.where(index > k, work - column * pivot, jnp.where(index == k, pivot, work))
        lower = jnp.where((across == k) & (down >= k), column[:, :edge], lower)
        for j in range(k + 1, edge):
            columns[j] = columns[j] - column * column[j : j + 1, :]
    return lower, jnp.where(down <= across, work[:, :edge], 0.0), work[:, edge:]


def combine(factor, data):
    rows = factor.shape[0]
    out = nn(jnp.concatenate([split3(factor)] * 3, axis=1), split3(data))
    return out[:rows] + out[rows : 2 * rows] + out[2 * rows :]


MM = functools.partial(nn, precision=HIGHEST)
MT = functools.partial(nt, precision=HIGHEST)


def prepare_body(groups, n_docs, n_terms, *refs):
    grams = refs[:groups]
    (out,) = refs[groups:]
    vectors = out.shape[1]
    low = grams[0][...]
    for ref in grams[1:]:
        low = low + ref[...]
    first = low[:, vectors : 2 * vectors]
    low = low[:, :vectors]
    _, _, inverse_zero = factorize(first / n_terms)
    lower_one, upper_one, inverse = factorize(MT(MM(inverse_zero, low / n_docs), inverse_zero))
    projection = upper_one * (n_docs / n_terms)
    values = (
        low,
        lower_one,
        projection,
        MT(projection, projection),
        MM(inverse, inverse_zero),
        MM(projection, inverse_zero),
    )
    for i, value in enumerate(values):
        out[i] = pad_lanes(value)


def prepare(n_docs, n_terms, grams):
    vectors = grams[0].shape[0]
    return pl.pallas_call(
        functools.partial(prepare_body, len(grams), n_docs, n_terms),
        in_specs=specs(*[VMEM] * len(grams)),
        out_specs=pl.BlockSpec(memory_space=VMEM),
        out_shape=VMEM((6, vectors, LANES), F32),
        compiler_params=SMALL,
        name="prepare",
    )(*inside(grams))


def finish_body(groups, n_docs, n_terms, *refs):
    grams = refs[:groups]
    ready, first, second, right_part, own = refs[groups : groups + 5]
    left_out, right_out, coefficients = refs[groups + 5 :]
    share, vectors, edge = right_part.shape
    gram = grams[0][...]
    for ref in grams[1:]:
        gram = gram + ref[...]
    cross = gram[:, :vectors]
    high = gram[:, vectors : 2 * vectors]
    low, lower_one, projection_one, square, both, back = [
        ready[i][:, :vectors] for i in range(6)
    ]
    lower_two, upper_two, inverse_two = factorize(MT(MM(both, cross / n_terms), both) - square)
    projection_two = upper_two * (n_terms / n_docs)
    main = MM(inverse_two, both)
    minus = MM(inverse_two, back)
    side = minus + MM(projection_two, both)
    right_factor = jnp.concatenate([main, -minus], axis=1)
    main_high = MM(main, high) - MT(side, cross)
    main_low = MM(main, cross) - MM(side, low)
    lower_three, _, inverse_three = factorize(
        (MT(main_high, main) - MT(main_low, side)) / n_docs
    )
    left_factor = jnp.concatenate([MM(inverse_three, main), -MM(inverse_three, side)], axis=1)
    for i, value in enumerate((lower_one, projection_one, lower_two, projection_two, lower_three)):
        coefficients[i] = value
    for t in range(share):
        data = jnp.concatenate([right_part[t], own[:, t * edge : (t + 1) * edge]], axis=0)
        right_out[:, t * edge : (t + 1) * edge] = combine(right_factor, data)
    for t in range(first.shape[0]):
        data = jnp.concatenate([second[t], first[t]], axis=0)
        left_out[:, t * edge : (t + 1) * edge] = combine(left_factor, data)


def finish(n_docs, n_terms, grams, ready, first, second, right_part, own):
    share, vectors, edge = right_part.shape
    return pl.pallas_call(
        functools.partial(finish_body, len(grams), n_docs, n_terms),
        in_specs=specs(*[VMEM] * (len(grams) + 5)),
        out_specs=specs(*[VMEM] * 3),
        out_shape=[
            jax.ShapeDtypeStruct((vectors, first.shape[0] * edge), F32),
            jax.ShapeDtypeStruct((vectors, share * edge), F32),
            jax.ShapeDtypeStruct((5, vectors, vectors), F32),
        ],
        compiler_params=SMALL,
        name="finish",
    )(*inside([*grams, ready, first, second, right_part, own]))


def shift(value, axis, step):
    size = lax.axis_size(axis)
    return lax.ppermute(value, axis, [(i, (i + step) % size) for i in range(size)])


def hop(value, mask, axis="term"):
    return lax.ppermute(value, axis, [(i, i ^ mask) for i in range(lax.axis_size(axis))])


def from_all(value, axis):
    return [value] + [shift(value, axis, k) for k in range(1, lax.axis_size(axis))]


def from_pairs(value, axis):
    size = lax.axis_size(axis)
    if size & (size - 1):
        return from_all(value, axis)
    held = [value]
    for k in range(1, size):
        held.append(hop(value, k, axis))
    return held


def around(low, high, axis):
    size = lax.axis_size(axis)
    lows, highs = {0: low}, {0: high}
    ahead, behind = (low, high), (low, high)
    for k in range(1, size // 2 + 1):
        if 2 * k < size:
            ahead = (shift(ahead[0], axis, 1), shift(ahead[1], axis, 1))
            behind = (shift(behind[0], axis, -1), shift(behind[1], axis, -1))
            lows[k], highs[k] = ahead
            lows[size - k], highs[size - k] = behind
        else:
            lows[k] = shift(ahead[0], axis, 1)
            highs[k] = shift(behind[1], axis, -1)
    return [half for k in range(size) for half in (lows[k], highs[k])]


STEPS = (
    ("low_x", "low", 2),
    ("high_y", "high", 4),
    ("high_x", "high", 2),
    ("low_y", "low", 4),
    ("whole_p", "whole", 1),
    ("low_d", "low_x", 4),
    ("high_d", "high_y", 2),
    ("low_x_p", "low_x", 1),
    ("high_y_p", "high_y", 1),
    ("high_x_p", "high_x", 1),
    ("low_y_p", "low_y", 1),
    ("high_d_p", "high_d", 1),
    ("low_d_p", "low_d", 1),
)


def term_gather(low, high, whole):
    if lax.axis_size("term") != 8:
        halves = [h for pair in zip(from_all(low, "term"), from_all(high, "term")) for h in pair]
        return halves, (0,) * len(halves)
    held = {"low": low, "high": high, "whole": whole}
    for name, source, mask in STEPS:
        held[name] = hop(held[source], mask)
    held["low_p"] = held["high_p"] = held["whole_p"]
    halves, offsets = [], []
    for end in ("", "_x", "_y", "_d", "_p", "_x_p", "_y_p", "_d_p"):
        halves += [held["low" + end], held["high" + end]]
        offsets += [0, low.shape[0] if end == "_p" else 0]
    return halves, tuple(offsets)


def after(values, first):
    return lax.optimization_barrier((values, first))[0]


def on_device(tiles, tile_rows, tile_cols, counts, start):
    return program(tiles[0, 0], tile_rows[0, 0], tile_cols[0, 0], counts[0], start)


def program(tiles, rows, cols, in_use, start):
    doc_groups = lax.axis_size("doc")
    term_groups = lax.axis_size("term")
    edge = tiles.shape[1]
    n_docs = DOC_TILES * edge * doc_groups
    n_terms = TERM_TILES * edge * term_groups
    row_share = DOC_TILES // term_groups
    col_share = TERM_TILES // doc_groups
    tiles, sums, picked, places = column_sums(tiles, start, cols, rows, in_use)
    all_sums = from_all(sums, "doc")
    own_part, own = own_gram(col_share * edge, after(start, sums))
    low, high, whole, col_scale = first_forward(tiles, picked, places, own_part, all_sums)
    dense, row_scale, low, high, where, own_part = backward(
        term_gather(low, high, whole), tiles, col_scale
    )
    halves = around(low, high, "doc")
    low_grams = from_pairs(low_gram(after(dense, halves[2]), own_part), "doc")
    low, high, whole, right_part = second_forward(
        col_share, tiles, col_scale, row_scale, all_sums, halves
    )
    gram, first, second = high_gram(row_share, where, term_gather(low, high, whole), dense)
    ready = prepare(n_docs, n_terms, after(low_grams, gram))
    grams = from_pairs(gram, "doc")
    return finish(n_docs, n_terms, grams, ready, first, second, right_part, own)


def solution(mesh):
    in_specs = (
        P("doc", "term", None, None, None),
        P("doc", "term", None),
        P("doc", "term", None),
        P("doc", "term"),
        P(None, "term"),
    )
    out_specs = (P(None, ("doc", "term")), P(None, ("term", "doc")), P())
    return jax.shard_map(
        on_device, mesh=mesh, in_specs=in_specs, out_specs=out_specs, check_vma=False
    )
```
